128 devices in a mesh: row: 8 (over y_hi, z), col: 16 (over x, y_lo, core).
Axes of the slice: x: 4, y: 4 (y_hi: 2, y_lo: 2; y = y_hi * 2 + y_lo), z: 4, core: 2. Of those that a mesh axis runs over, the one named last changes fastest.
Arguments:
- response_coeffs: float32 [3, 8192, 1024], P(None, ('row', 'col')), may hold values from -6 to 6
- occupied_coeffs: float32 [8192, 1024], P(('row', 'col')), may hold values from -0.1875 to 0.1875
Outputs:
- density: float32 [3, 8192, 8192], P(None, 'row', 'col')
The draws below stay inside these ranges and needn't reach their ends.
All inputs are finite; a program needn't handle non-finite values.
Results may differ from the reference program's by a relative error of at most 0.0003.
Values sent between devices are 32-bit elements; how exact they have to be, the bound alone decides.
No kernel may reach another device: no remote copies, remote signals or barrier semaphores. Data moves between devices by JAX's collectives and lax.ppermute only.
A program may use at most 128 MiB of HBM per device.

```python
import jax
import jax.numpy as jnp
from jax import lax

BASIS = 8192
OCC = 1024
PERTURB = 3


def level_of(key, dims, split, low, top_value):
    gain, own = 1.0, jax.random.fold_in(key, 6)
    for dim, blocks in split:
        heights = jnp.exp(jax.random.uniform(jax.random.fold_in(own, dim), (blocks,), jnp.float32, low / len(split), top_value / len(split)))
        gain = gain * jnp.repeat(heights, dims[dim] // blocks).reshape([-1 if axis == dim else 1 for axis in range(len(dims))])
    return gain


def normal_values(rng, shape, deviation, most, pieces=(), dtype=jnp.bfloat16):
    values = deviation * jax.random.normal(rng, shape, jnp.float32)
    if pieces:
        values = values * level_of(rng, shape, pieces, -0.22, 0.18)
    return jnp.clip(values, -most, most).astype(dtype)


def setup_inputs(seed: int = 0) -> dict:
    keys = jax.random.split(jax.random.key(seed), 3)
    response_coeffs = normal_values(keys[0], (PERTURB, BASIS, OCC), 1.0, 6.0, ((1, 128),), jnp.float32)
    occupied_coeffs = normal_values(keys[1], (BASIS, OCC), OCC ** -0.5, 0.1875, ((0, 128),), jnp.float32)
    return dict(response_coeffs=response_coeffs, occupied_coeffs=occupied_coeffs)


SLICE_PAIRS = ((0, 0), (0, 1), (1, 0))


def split_slices(values):
    leading = lax.optimization_barrier(values.astype(jnp.bfloat16))
    remainder = values - leading.astype(jnp.float32)
    trailing = lax.optimization_barrier(remainder.astype(jnp.bfloat16))
    return [leading, trailing]


def reference(response_coeffs, occupied_coeffs):
    response_slices = split_slices(response_coeffs)
    occupied_slices = split_slices(occupied_coeffs)
    accumulated = jnp.zeros((PERTURB, BASIS, BASIS), jnp.float32)
    for left_index, right_index in SLICE_PAIRS:
        accumulated = accumulated + jnp.einsum(
            "kno,mo->knm",
            response_slices[left_index].astype(jnp.float32),
            occupied_slices[right_index].astype(jnp.float32),
            precision=lax.Precision.HIGHEST,
        )
    return accumulated + jnp.swapaxes(accumulated, 1, 2)
```

```python
import functools

import jax
import jax.numpy as jnp
from jax import lax
from jax.experimental import pallas as pl
from jax.experimental.pallas import tpu as pltpu
from jax.sharding import PartitionSpec as P


AXES = ("row", "col")
PIECES = ((0, 512), (512, 512))


def place(index):
    row, col = divmod(index, 16)
    y_hi, z = divmod(row, 4)
    x, rest = divmod(col, 4)
    y_lo, core = divmod(rest, 2)
    return x, y_hi, y_lo, z, core


def index_of(x, y_hi, y_lo, z, core):
    return (y_hi % 2 * 4 + z % 4) * 16 + x % 4 * 4 + y_lo % 2 * 2 + core % 2


def move(value, target):
    pairs = [(source, index_of(*target(*place(source)))) for source in range(128)]
    return lax.ppermute(value, AXES, pairs)


def gather_rows(own):
    step_x = lambda d: lambda x, h, l, z, k: (x + d, h, l, z, k)
    pair = move(own, lambda x, h, l, z, k: (x, h, l + 1, z, k))
    own_minus = move(own, step_x(1))
    own_plus = move(own, step_x(-1))
    pair_minus = move(pair, step_x(1))
    pair_plus = move(pair, step_x(-1))
    own_far = move(own_minus, step_x(1))
    pair_far = move(pair_plus, step_x(-1))
    chunks = (own, pair, own_minus, pair_minus, own_plus, pair_plus, own_far, pair_far)
    swap = lambda x, h, l, z, k: (x, h, l, z, k + 1)
    return [(chunk, move(chunk, swap)) for chunk in chunks]


def gather_columns(own):
    step_z = lambda d: lambda x, h, l, z, k: (x, h, l, z + d, k)
    shifted = move(own, lambda x, h, l, z, k: (x, h, l, z + 2 * k + l, k))

    def into_column(x, h, l, z, k):
        source = (z - 2 * k - l) % 4
        return 2 * h + source // 2, x % 2, source % 2, z, x // 2

    entry = move(shifted, into_column)
    other = move(entry, lambda x, h, l, z, k: (x, h + 1, l, z, k))
    entry_minus = move(entry, step_z(1))
    entry_plus = move(entry, step_z(-1))
    other_minus = move(other, step_z(1))
    other_plus = move(other, step_z(-1))
    entry_far = move(entry_minus, step_z(1))
    other_far = move(other_plus, step_z(-1))
    return (
        (entry, entry_minus, entry_plus, entry_far),
        (other, other_minus, other_plus, other_far),
    )


OFFSETS = (0, 3, 1, 2)
CALLS = (((0, 2), (2, 4)), ((0, 2), (2, 4)))


def split(value):
    high = value.astype(jnp.bfloat16)
    low = (value - high.astype(jnp.float32)).astype(jnp.bfloat16)
    return high, low


def density_kernel(add, tiles, tile_ref, within_ref, slot_ref, *refs):
    rows, columns, refs = refs[: 4 * tiles], refs[4 * tiles : 4 * tiles + 8], refs[4 * tiles + 8 :]
    if add is not None:
        before, refs = refs[0], refs[1:]
    out, row_full, col_full, row_high, row_low, col_high, col_low, held, made = refs[:9]
    row_sem, col_sem, held_sem, made_sem = refs[9:]
    _, mats, height, depth = row_full.shape
    count, last = 4 * height, mats - 1

    def block(ref, t):
        start = pl.multiple_of(tile_ref[t] * count, count)
        return ref.at[:, pl.ds(start, count), :]

    def fetch_rows(i, source):
        return pltpu.make_async_copy(source, row_full.at[i], row_sem.at[i])

    def fetch_held(t):
        return pltpu.make_async_copy(block(before, t), held.at[t], held_sem.at[t])

    def store(t):
        slot = lax.rem(t, 2)
        return pltpu.make_async_copy(made.at[slot], block(out, t), made_sem.at[slot])

    copies = []
    for n, column in enumerate(columns):
        copies.append(pltpu.make_async_copy(column, col_full.at[n], col_sem.at[n]))
        copies[-1].start()
    for t in range(tiles):
        for i in range(4 * t, 4 * t + 4):
            fetch_rows(i, rows[i]).start()
        if add:
            fetch_held(t).start()
    for n, copy in enumerate(copies):
        copy.wait()
        slot = slot_ref[n]
        high, low = split(col_full[n])
        col_high[:, slot] = high
        col_low[:, slot] = low

    dims = (((1,), (1,)), ((), ()))
    dot = lambda u, v: lax.dot_general(u, v, dims, preferred_element_type=jnp.float32)
    row = lambda ref, k: ref[k].reshape(count, depth)
    col = lambda ref, k: ref[k].reshape(8 * height, depth)

    def step(t, carry):
        for n in range(4):
            i = 4 * t + n
            fetch_rows(i, rows[n]).wait()
            high, low = split(row_full[i])
            row_high[:, n ^ within_ref[0]] = high
            row_low[:, n ^ within_ref[0]] = low
        if add:
            fetch_held(t).wait()

        @pl.when(t >= 2)
        def _():
            store(t - 2).wait()

        for k in range(last):
            total = (
                dot(row(row_high, k), col(col_high, last))
                + dot(row(row_high, last), col(col_high, k))
                + dot(row(row_high, k), col(col_low, last))
                + dot(row(row_low, k), col(col_high, last))
                + dot(row(row_high, last), col(col_low, k))
                + dot(row(row_low, last), col(col_high, k))
            )
            if add:
                total = total + held[t, k]
            made[lax.rem(t, 2), k] = total
        store(t).start()
        return carry

    lax.fori_loop(0, tiles, step, 0)
    for t in range(max(tiles - 2, 0), tiles):
        store(t).wait()


def add_tiles(rows, columns, where, within, slots, before, add):
    tiles = len(rows) // 4
    mats, height, depth = rows[0].shape
    count, width = 4 * height, 8 * height
    operands = [*rows, *columns]
    if before is None:
        add = None
    else:
        operands.append(before)
    vmem = lambda shape, dtype: pltpu.VMEM(shape, dtype)
    return pl.pallas_call(
        functools.partial(density_kernel, add, tiles),
        out_shape=jax.ShapeDtypeStruct((mats - 1, 4 * count, width), jnp.float32),
        grid_spec=pltpu.PrefetchScalarGridSpec(
            num_scalar_prefetch=3,
            grid=(1,),
            in_specs=[pl.BlockSpec(memory_space=pltpu.HBM)] * len(operands),
            out_specs=pl.BlockSpec(memory_space=pltpu.HBM),
            scratch_shapes=[
                vmem((4 * tiles, mats, height, depth), jnp.float32),
                vmem((8, mats, height, depth), jnp.float32),
                vmem((mats, 4, height, depth), jnp.bfloat16),
                vmem((mats, 4, height, depth), jnp.bfloat16),
                vmem((mats, 8, height, depth), jnp.bfloat16),
                vmem((mats, 8, height, depth), jnp.bfloat16),
                vmem((tiles if add else 1, mats - 1, count, width), jnp.float32),
                vmem((2, mats - 1, count, width), jnp.float32),
                pltpu.SemaphoreType.DMA((4 * tiles,)),
                pltpu.SemaphoreType.DMA((8,)),
                pltpu.SemaphoreType.DMA((4,)),
                pltpu.SemaphoreType.DMA((2,)),
            ],
        ),
        input_output_aliases={} if before is None else {2 + len(operands): 0},
        cost_estimate=pl.CostEstimate(
            flops=2 * 6 * (mats - 1) * tiles * count * width * depth,
            bytes_accessed=(len(rows) + 8) * mats * height * depth * 4,
            transcendentals=0,
        ),
    )(where, within, slots, *operands)


def whole(response_coeffs, occupied_coeffs):
    own = jnp.concatenate([response_coeffs, occupied_coeffs[None]], axis=0)
    row, col = lax.axis_index("row"), lax.axis_index("col")
    x, pair = col // 4, col % 4
    y_hi, z = row // 4, row % 4
    source = (x % 2) * 2 + pair // 2
    parts = [own[:, :, s : s + d] for s, d in PIECES]
    columns = [gather_columns(part) for part in parts]
    tiles = [gather_rows(part) for part in parts]
    turn = (z + jnp.array(OFFSETS) - source) % 4
    base = turn % 2 * 2 + turn // 2
    slots = jnp.concatenate([y_hi * 4 + base, (1 - y_hi) * 4 + base]).astype(jnp.int32)
    where = ((x + jnp.array(OFFSETS)) % 4).astype(jnp.int32)
    within = pair[None].astype(jnp.int32)
    density = None
    for n, (entry, other) in enumerate(columns):
        for start, stop in CALLS[n]:
            rows = sum(tiles[n][2 * start : 2 * stop], ())
            density = add_tiles(
                rows,
                (*entry, *other),
                where[start:stop],
                within,
                slots,
                density,
                n > 0,
            )
    return density


def solution(mesh):
    return jax.shard_map(
        whole,
        mesh=mesh,
        in_specs=(P(None, ("row", "col"), None), P(("row", "col"), None)),
        out_specs=P(None, "row", "col"),
        check_vma=False,
    )
```

```python
import functools

import jax
import jax.numpy as jnp
from jax import lax
from jax.experimental import pallas as pl
from jax.experimental.pallas import tpu as pltpu
from jax.sharding import PartitionSpec as P


AXES = ("row", "col")
PIECES = ((0, 512), (512, 512))


def place(index):
    row, col = divmod(index, 16)
    y_hi, z = divmod(row, 4)
    x, rest = divmod(col, 4)
    y_lo, core = divmod(rest, 2)
    return x, y_hi, y_lo, z, core


def index_of(x, y_hi, y_lo, z, core):
    return (y_hi % 2 * 4 + z % 4) * 16 + x % 4 * 4 + y_lo % 2 * 2 + core % 2


def move(value, target):
    pairs = [(source, index_of(*target(*place(source)))) for source in range(128)]
    return lax.ppermute(value, AXES, pairs)


def gather_rows(own):
    step_x = lambda d: lambda x, h, l, z, k: (x + d, h, l, z, k)
    pair = move(own, lambda x, h, l, z, k: (x, h, l + 1, z, k))
    own_minus = move(own, step_x(1))
    own_plus = move(own, step_x(-1))
    pair_minus = move(pair, step_x(1))
    pair_plus = move(pair, step_x(-1))
    own_far = move(own_minus, step_x(1))
    pair_far = move(pair_plus, step_x(-1))
    chunks = (own, pair, own_minus, pair_minus, own_plus, pair_plus, own_far, pair_far)
    swap = lambda x, h, l, z, k: (x, h, l, z, k + 1)
    return [(chunk, move(chunk, swap)) for chunk in chunks]


def gather_columns(own):
    step_z = lambda d: lambda x, h, l, z, k: (x, h, l, z + d, k)
    shifted = move(own, lambda x, h, l, z, k: (x, h, l, z + 2 * k + l, k))

    def into_column(x, h, l, z, k):
        source = (z - 2 * k - l) % 4
        return 2 * h + source // 2, x % 2, source % 2, z, x // 2

    entry = move(shifted, into_column)
    other = move(entry, lambda x, h, l, z, k: (x, h + 1, l, z, k))
    entry_minus = move(entry, step_z(1))
    entry_plus = move(entry, step_z(-1))
    other_minus = move(other, step_z(1))
    other_plus = move(other, step_z(-1))
    entry_far = move(entry_minus, step_z(1))
    other_far = move(other_plus, step_z(-1))
    return (
        (entry, entry_minus, entry_plus, entry_far),
        (other, other_minus, other_plus, other_far),
    )


OFFSETS = (0, 3, 1, 2)
CALLS = (((0, 2), (2, 4)), ((0, 4),))


def split(value):
    high = value.astype(jnp.bfloat16)
    low = (value - high.astype(jnp.float32)).astype(jnp.bfloat16)
    return high, low


def density_kernel(add, first, tiles, *refs):
    row, col = lax.axis_index("row"), lax.axis_index("col")
    x, pair = lax.div(col, 4), lax.rem(col, 4)
    y_hi, z = lax.div(row, 4), lax.rem(row, 4)
    source = lax.rem(x, 2) * 2 + lax.div(pair, 2)

    def slot_of(n):
        turn = lax.rem(z + OFFSETS[n % 4] + 4 - source, 4)
        base = lax.rem(turn, 2) * 2 + lax.div(turn, 2)
        return (y_hi if n < 4 else 1 - y_hi) * 4 + base

    rows, columns, refs = refs[: 4 * tiles], refs[4 * tiles : 4 * tiles + 8], refs[4 * tiles + 8 :]
    if add is not None:
        before, refs = refs[0], refs[1:]
    out, row_full, col_full, row_high, row_low, col_high, col_low, held, made = refs[:9]
    row_sem, col_sem, held_sem, made_sem = refs[9:]
    _, mats, height, depth = row_full.shape
    count, last = 4 * height, mats - 1

    def block(ref, t):
        t = t + first
        offset = jnp.where(t == 0, 0, jnp.where(t == 1, 3, t - 1))
        start = pl.multiple_of(lax.rem(x + offset, 4) * count, count)
        return ref.at[:, pl.ds(start, count), :]

    def fetch_rows(i, source):
        return pltpu.make_async_copy(source, row_full.at[i], row_sem.at[i])

    def fetch_held(t):
        return pltpu.make_async_copy(block(before, t), held.at[t], held_sem.at[t])

    def store(t):
        slot = lax.rem(t, 2)
        return pltpu.make_async_copy(made.at[slot], block(out, t), made_sem.at[slot])

    copies = []
    for n, column in enumerate(columns):
        copies.append(pltpu.make_async_copy(column, col_full.at[n], col_sem.at[n]))
        copies[-1].start()
    for t in range(tiles):
        for i in range(4 * t, 4 * t + 4):
            fetch_rows(i, rows[i]).start()
        if add:
            fetch_held(t).start()
    for n, copy in enumerate(copies):
        copy.wait()
        slot = slot_of(n)
        high, low = split(col_full[n])
        col_high[:, slot] = high
        col_low[:, slot] = low

    dims = (((1,), (1,)), ((), ()))
    dot = lambda u, v: lax.dot_general(u, v, dims, preferred_element_type=jnp.float32)
    row = lambda ref, k: ref[k].reshape(count, depth)
    col = lambda ref, k: ref[k].reshape(8 * height, depth)

    def step(t, carry):
        for n in range(4):
            i = 4 * t + n
            fetch_rows(i, rows[n]).wait()
            high, low = split(row_full[i])
            row_high[:, n ^ pair] = high
            row_low[:, n ^ pair] = low
        if add:
            fetch_held(t).wait()

        @pl.when(t >= 2)
        def _():
            store(t - 2).wait()

        for k in range(last):
            total = (
                dot(row(row_high, k), col(col_high, last))
                + dot(row(row_high, last), col(col_high, k))
                + dot(row(row_high, k), col(col_low, last))
                + dot(row(row_low, k), col(col_high, last))
                + dot(row(row_high, last), col(col_low, k))
                + dot(row(row_low, last), col(col_high, k))
            )
            if add:
                total = total + held[t, k]
            made[lax.rem(t, 2), k] = total
        store(t).start()
        return carry

    lax.fori_loop(0, tiles, step, 0)
    for t in range(max(tiles - 2, 0), tiles):
        store(t).wait()


def add_tiles(rows, columns, first, before, add):
    tiles = len(rows) // 4
    mats, height, depth = rows[0].shape
    count, width = 4 * height, 8 * height
    operands = [*rows, *columns]
    if before is None:
        add = None
    else:
        operands.append(before)
    vmem = lambda shape, dtype: pltpu.VMEM(shape, dtype)
    return pl.pallas_call(
        functools.partial(density_kernel, add, first, tiles),
        out_shape=jax.ShapeDtypeStruct((mats - 1, 4 * count, width), jnp.float32),
        grid_spec=pltpu.PrefetchScalarGridSpec(
            num_scalar_prefetch=0,
            grid=(1,),
            in_specs=[pl.BlockSpec(memory_space=pltpu.HBM)] * len(operands),
            out_specs=pl.BlockSpec(memory_space=pltpu.HBM),
            scratch_shapes=[
                vmem((4 * tiles, mats, height, depth), jnp.float32),
                vmem((8, mats, height, depth), jnp.float32),
                vmem((mats, 4, height, depth), jnp.bfloat16),
                vmem((mats, 4, height, depth), jnp.bfloat16),
                vmem((mats, 8, height, depth), jnp.bfloat16),
                vmem((mats, 8, height, depth), jnp.bfloat16),
                vmem((tiles if add else 1, mats - 1, count, width), jnp.float32),
                vmem((2, mats - 1, count, width), jnp.float32),
                pltpu.SemaphoreType.DMA((4 * tiles,)),
                pltpu.SemaphoreType.DMA((8,)),
                pltpu.SemaphoreType.DMA((4,)),
                pltpu.SemaphoreType.DMA((2,)),
            ],
        ),
        input_output_aliases={} if before is None else {len(operands) - 1: 0},
        cost_estimate=pl.CostEstimate(
            flops=2 * 6 * (mats - 1) * tiles * count * width * depth,
            bytes_accessed=(len(rows) + 8) * mats * height * depth * 4,
            transcendentals=0,
        ),
    )(*operands)


def whole(response_coeffs, occupied_coeffs):
    parts = [
        jnp.concatenate(
            [response_coeffs[:, :, s : s + d], occupied_coeffs[None, :, s : s + d]]
        )
        for s, d in PIECES
    ]
    columns = [gather_columns(part) for part in parts]
    tiles = [gather_rows(part) for part in parts]
    density = None
    for n, (entry, other) in enumerate(columns):
        for start, stop in CALLS[n]:
            rows = sum(tiles[n][2 * start : 2 * stop], ())
            density = add_tiles(
                rows, (*entry, *other), start, density, n > 0
            )
    return density


def solution(mesh):
    return jax.shard_map(
        whole,
        mesh=mesh,
        in_specs=(P(None, ("row", "col"), None), P(("row", "col"), None)),
        out_specs=P(None, "row", "col"),
        check_vma=False,
    )
```

```python
import functools

import jax
import jax.numpy as jnp
from jax import lax
from jax.experimental import pallas as pl
from jax.experimental.pallas import tpu as pltpu
from jax.sharding import PartitionSpec as P


AXES = ("row", "col")
PIECES = ((0, 512), (512, 512))


def place(index):
    row, col = divmod(index, 16)
    y_hi, z = divmod(row, 4)
    x, rest = divmod(col, 4)
    y_lo, core = divmod(rest, 2)
    return x, y_hi, y_lo, z, core


def index_of(x, y_hi, y_lo, z, core):
    return (y_hi % 2 * 4 + z % 4) * 16 + x % 4 * 4 + y_lo % 2 * 2 + core % 2


def move(value, target):
    pairs = [(source, index_of(*target(*place(source)))) for source in range(128)]
    return lax.ppermute(value, AXES, pairs)


def gather_rows(own):
    step_x = lambda d: lambda x, h, l, z, k: (x + d, h, l, z, k)
    pair = move(own, lambda x, h, l, z, k: (x, h, l + 1, z, k))
    own_minus = move(own, step_x(1))
    own_plus = move(own, step_x(-1))
    pair_minus = move(pair, step_x(1))
    pair_plus = move(pair, step_x(-1))
    own_far = move(own_minus, step_x(1))
    pair_far = move(pair_plus, step_x(-1))
    chunks = (own, pair, own_minus, pair_minus, own_plus, pair_plus, own_far, pair_far)
    swap = lambda x, h, l, z, k: (x, h, l, z, k + 1)
    return [(chunk, move(chunk, swap)) for chunk in chunks]


def gather_columns(tag, own):
    step_z = lambda d: lambda x, h, l, z, k: (x, h, l, z + d, k)
    shifted = move(own, lambda x, h, l, z, k: (x, h, l, z + 2 * k + l, k))

    def into_column(x, h, l, z, k):
        source = (z - 2 * k - l) % 4
        return 2 * h + source // 2, x % 2, source % 2, z, x // 2

    entry = move(shifted, into_column)
    other = move(entry, lambda x, h, l, z, k: (x, h + 1, l, z, k))
    entry_minus = move(entry, step_z(1))
    entry_plus = move(entry, step_z(-1))
    other_minus = move(other, step_z(1))
    other_plus = move(other, step_z(-1))
    entry_far = move(entry_minus, step_z(1))
    if tag == "0":
        other_far = move(other_plus, step_z(-1))
    else:
        partner = lambda x, h, l, z, k: (x, h + 1, l, z, k)
        other_far = move(entry_far, partner)
    return (
        (entry, entry_minus, entry_plus, entry_far),
        (other, other_minus, other_plus, other_far),
    )


OFFSETS = (0, 3, 1, 2)
CALLS = (((0, 2), (2, 4)), ((0, 4),))


def split(value):
    high = value.astype(jnp.bfloat16)
    low = (value - high.astype(jnp.float32)).astype(jnp.bfloat16)
    return high, low


def density_kernel(add, first, tiles, *refs):
    row, col = lax.axis_index("row"), lax.axis_index("col")
    x, pair = lax.div(col, 4), lax.rem(col, 4)
    y_hi, z = lax.div(row, 4), lax.rem(row, 4)
    source = lax.rem(x, 2) * 2 + lax.div(pair, 2)

    def slot_of(n):
        turn = lax.rem(z + OFFSETS[n % 4] + 4 - source, 4)
        base = lax.rem(turn, 2) * 2 + lax.div(turn, 2)
        return (y_hi if n < 4 else 1 - y_hi) * 4 + base

    rows, columns, refs = refs[: 4 * tiles], refs[4 * tiles : 4 * tiles + 8], refs[4 * tiles + 8 :]
    if add is not None:
        before, refs = refs[0], refs[1:]
    out, row_full, col_full, row_high, row_low, col_high, col_low, held, made = refs[:9]
    row_sem, col_sem, held_sem, made_sem = refs[9:]
    _, mats, height, depth = row_full.shape
    count, last = 4 * height, mats - 1

    def block(ref, t):
        t = t + first
        offset = jnp.where(t == 0, 0, jnp.where(t == 1, 3, t - 1))
        start = pl.multiple_of(lax.rem(x + offset, 4) * count, count)
        return ref.at[:, pl.ds(start, count), :]

    def fetch_rows(i, source):
        return pltpu.make_async_copy(source, row_full.at[i], row_sem.at[i])

    def fetch_held(t):
        return pltpu.make_async_copy(block(before, t), held.at[t], held_sem.at[t])

    def store(t):
        slot = lax.rem(t, 2)
        return pltpu.make_async_copy(made.at[slot], block(out, t), made_sem.at[slot])

    copies = []
    for n, column in enumerate(columns):
        copies.append(pltpu.make_async_copy(column, col_full.at[n], col_sem.at[n]))
        copies[-1].start()
    for t in range(tiles):
        for i in range(4 * t, 4 * t + 4):
            fetch_rows(i, rows[i]).start()
        if add:
            fetch_held(t).start()
    for n, copy in enumerate(copies):
        copy.wait()
        slot = slot_of(n)
        high, low = split(col_full[n])
        col_high[:, slot] = high
        col_low[:, slot] = low

    dims = (((1,), (1,)), ((), ()))
    dot = lambda u, v: lax.dot_general(u, v, dims, preferred_element_type=jnp.float32)
    row = lambda ref, k: ref[k].reshape(count, depth)
    col = lambda ref, k: ref[k].reshape(8 * height, depth)

    def step(t, carry):
        for n in range(4):
            i = 4 * t + n
            fetch_rows(i, rows[n]).wait()
            high, low = split(row_full[i])
            row_high[:, n ^ pair] = high
            row_low[:, n ^ pair] = low
        if add:
            fetch_held(t).wait()

        @pl.when(t >= 2)
        def _():
            store(t - 2).wait()

        for k in range(last):
            total = (
                dot(row(row_high, k), col(col_high, last))
                + dot(row(row_high, last), col(col_high, k))
                + dot(row(row_high, k), col(col_low, last))
                + dot(row(row_low, k), col(col_high, last))
                + dot(row(row_high, last), col(col_low, k))
                + dot(row(row_low, last), col(col_high, k))
            )
            if add:
                total = total + held[t, k]
            made[lax.rem(t, 2), k] = total
        store(t).start()
        return carry

    lax.fori_loop(0, tiles, step, 0)
    for t in range(max(tiles - 2, 0), tiles):
        store(t).wait()


def add_tiles(rows, columns, first, before, add):
    tiles = len(rows) // 4
    mats, height, depth = rows[0].shape
    count, width = 4 * height, 8 * height
    operands = [*rows, *columns]
    if before is None:
        add = None
    else:
        operands.append(before)
    vmem = lambda shape, dtype: pltpu.VMEM(shape, dtype)
    return pl.pallas_call(
        functools.partial(density_kernel, add, first, tiles),
        out_shape=jax.ShapeDtypeStruct((mats - 1, 4 * count, width), jnp.float32),
        grid_spec=pltpu.PrefetchScalarGridSpec(
            num_scalar_prefetch=0,
            grid=(1,),
            in_specs=[pl.BlockSpec(memory_space=pltpu.HBM)] * len(operands),
            out_specs=pl.BlockSpec(memory_space=pltpu.HBM),
            scratch_shapes=[
                vmem((4 * tiles, mats, height, depth), jnp.float32),
                vmem((8, mats, height, depth), jnp.float32),
                vmem((mats, 4, height, depth), jnp.bfloat16),
                vmem((mats, 4, height, depth), jnp.bfloat16),
                vmem((mats, 8, height, depth), jnp.bfloat16),
                vmem((mats, 8, height, depth), jnp.bfloat16),
                vmem((tiles if add else 1, mats - 1, count, width), jnp.float32),
                vmem((2, mats - 1, count, width), jnp.float32),
                pltpu.SemaphoreType.DMA((4 * tiles,)),
                pltpu.SemaphoreType.DMA((8,)),
                pltpu.SemaphoreType.DMA((4,)),
                pltpu.SemaphoreType.DMA((2,)),
            ],
        ),
        input_output_aliases={} if before is None else {len(operands) - 1: 0},
        cost_estimate=pl.CostEstimate(
            flops=2 * 6 * (mats - 1) * tiles * count * width * depth,
            bytes_accessed=(len(rows) + 8) * mats * height * depth * 4,
            transcendentals=0,
        ),
    )(*operands)


def whole(response_coeffs, occupied_coeffs):
    parts = [
        jnp.concatenate(
            [response_coeffs[:, :, s : s + d], occupied_coeffs[None, :, s : s + d]]
        )
        for s, d in PIECES
    ]
    columns = [gather_columns(str(n), part) for n, part in enumerate(parts)]
    tiles = [gather_rows(part) for part in parts]
    density = None
    for n, (entry, other) in enumerate(columns):
        for start, stop in CALLS[n]:
            rows = sum(tiles[n][2 * start : 2 * stop], ())
            density = add_tiles(
                rows, (*entry, *other), start, density, n > 0
            )
    return density


def solution(mesh):
    return jax.shard_map(
        whole,
        mesh=mesh,
        in_specs=(P(None, ("row", "col"), None), P(("row", "col"), None)),
        out_specs=P(None, "row", "col"),
        check_vma=False,
    )
```
